32 devices in a mesh: seq: 16 (over z, y, core), batch: 2 (over x).
Axes of the slice: x: 2, y: 2, z: 4, core: 2. Of those that a mesh axis runs over, the one named last changes fastest.
Arguments:
- hidden_in: bfloat16 [2, 4096, 2304], P('batch', 'seq'), may hold values from -6 to 6
- segment_ids: int32 [2, 4096], P('batch', 'seq'), may hold values from 0 to 15, never falling along the last dimension, each value on 1 to 512 neighbouring positions
- pre_gain: float32 [2304], replicated, may hold values from 0.25 to 1.75
- w_qkv: bfloat16 [2304, 2048], P('seq'), may hold values from -0.27083333 to 0.27083333
- w_out: bfloat16 [1024, 2304], P('seq'), may hold values from -0.1875 to 0.1875
- post_gain: float32 [2304], replicated, may hold values from 0.25 to 1.75
Outputs:
- layer_out: bfloat16 [2, 4096, 2304], P('batch', 'seq')
The draws below stay inside these ranges and needn't reach their ends.
Inputs may be any that keep to these rules, and one draw needn't show every extreme that they name: `segment_ids`: along each sequence the numbers never fall; a document is 1 to 512 positions long, and each sequence has one of exactly 512.
All inputs are finite; a program needn't handle non-finite values.
Results may differ from the reference program's by a relative error of at most 0.012.
The reference program's roundings to bfloat16 on the way (of `normed` and `attended`) count: a program that leaves them out, or rounds other values in their place, can miss the bound.
Values may be sent and summed in bfloat16 or wider, within the bound.
A program may use at most 128 MiB of HBM per device.

```python
import math
import jax
import jax.numpy as jnp
import numpy as np
from jax import lax

D = 2304
Q_HEADS = 4
KV_HEADS = 2
HEAD = 256
WINDOW = 4096
DOCS = 16
TOK_DEV = 256
SEQ = 4096
BATCH = 2
QKV_W = 2048
ATT_W = 1024
DOC_MOST = 512


def draw_w_qkv(key, part):
    base_key = jax.random.fold_in(key, 11)
    pick_key = jax.random.fold_in(key, 12)
    base = jnp.clip(jax.random.normal(base_key, (D, QKV_W), jnp.float32), -3.0, 3.0)
    order = jax.random.permutation(pick_key, KV_HEADS)
    boosted = order < (KV_HEADS + 1) // 2
    columns = jnp.arange(QKV_W, dtype=jnp.int32)
    head_of = columns // HEAD
    group_of = jnp.where(head_of < Q_HEADS, head_of // (Q_HEADS // KV_HEADS), head_of - Q_HEADS)
    group_of = jnp.clip(group_of, 0, KV_HEADS - 1)
    is_value = head_of >= Q_HEADS + KV_HEADS
    factor = jnp.where(boosted[group_of] & jnp.logical_not(is_value), 4.0, 1.0).astype(jnp.float32)
    return (base * factor[None, :] * float(D) ** (-0.5)).astype(jnp.bfloat16)


def block_levels(stream_key, dims, cuts, least, high):
    def one(position, shards_of):
        steps = jax.random.uniform(jax.random.fold_in(jax.random.fold_in(stream_key, 6), position), (shards_of,), jnp.float32, least / len(cuts), high / len(cuts))
        return jnp.repeat(jnp.exp(steps), dims[position] // shards_of).reshape((-1,) + (1,) * (len(dims) - position - 1))

    factor_of = one(*cuts[0])
    for cut in cuts[1:]:
        factor_of = factor_of * one(*cut)
    return factor_of


def profile(count, total, limit, lean):
    weights = [(1 << 20) // math.isqrt(standing ** lean) + 1 for standing in range(2, count + 1)]
    rest, given = total - limit - (count - 1), [1] * (count - 1)
    while rest > 0:
        free = [i for i in range(count - 1) if given[i] < limit]
        whole, budget = sum([weights[i] for i in free]), rest
        for i in free:
            addition = min(limit - given[i], max(1, budget * weights[i] // whole), rest)
            given[i] = given[i] + addition
            rest = rest - addition
    return np.array([limit] + given)


def uneven(own_key, count, total, bound, skew):
    if count == 2:
        one = jax.random.randint(own_key, (), max(1, total - bound), min(bound, total - 1) + 1)
        return jnp.stack([one, total - one])
    sizes = jnp.asarray(profile(count, total, bound, skew), jnp.int32)
    pairs = (count - 1) // 2
    source_of, taker = sizes[1:1 + 2 * pairs:2], sizes[2:2 + 2 * pairs:2]
    margin = jnp.minimum(source_of - 1, bound - taker)
    passed = jax.random.randint(jax.random.fold_in(own_key, 1), (pairs,), 0, 1 << 20) % (margin + 1)
    sizes = sizes.at[1:1 + 2 * pairs:2].set(source_of - passed).at[2:2 + 2 * pairs:2].set(taker + passed)
    return sizes[jax.random.permutation(jax.random.fold_in(own_key, 2), count)]


def normal_values(own_key, dims, width, most, cuts=(), held_as=jnp.bfloat16):
    values = jax.random.normal(own_key, dims, jnp.float32) * width
    if len(cuts) > 0:
        values = block_levels(own_key, dims, cuts, -0.22, 0.18) * values
    return jnp.clip(values, min=-most, max=most).astype(held_as)


def setup_inputs(seed: int = 0) -> dict:
    arg_keys = jax.random.split(jax.random.key(seed), 7)
    hidden_in = normal_values(arg_keys[0], (BATCH, SEQ, D), 1.0, 6.0, ((0, 2), (1, 16)))
    segment_ids = jax.vmap(lambda own: jnp.searchsorted(jnp.cumsum(uneven(own, DOCS, SEQ, DOC_MOST, 2)), jnp.arange(SEQ), side="right"))(jax.random.split(arg_keys[1], BATCH)).reshape((BATCH, SEQ)).astype(jnp.int32)
    pre_gain = jnp.clip(1.0 + 0.15 * jax.random.normal(arg_keys[2], (D,), jnp.float32), 0.25, 1.75)
    w_qkv = draw_w_qkv(jax.random.fold_in(arg_keys[6], 71), 0)
    w_out = normal_values(arg_keys[4], (ATT_W, D), ATT_W ** -0.5, 0.1875, ((0, 16),))
    post_gain = jnp.clip(1.0 + 0.15 * jax.random.normal(arg_keys[5], (D,), jnp.float32), 0.25, 1.75)
    return dict(hidden_in=hidden_in, segment_ids=segment_ids, pre_gain=pre_gain, w_qkv=w_qkv, w_out=w_out, post_gain=post_gain)


EPS = 1e-06
CAP = 50.0

def rms_scale(values, gain):
    return values * lax.rsqrt(lax.optimization_barrier(jnp.mean(values * values, axis=-1, keepdims=True)) + EPS) * gain

def barrier_round(values):
    return lax.optimization_barrier(values.astype(jnp.bfloat16)).astype(jnp.float32)

def rotary(values, positions):
    head_size = values.shape[-1]
    half_dim = head_size // 2
    inverse = 1.0 / 10000.0 ** (jnp.arange(half_dim, dtype=jnp.float32) * 2.0 / head_size)
    angles = positions.astype(jnp.float32)[:, None] * inverse[None, :]
    shape = (values.shape[0],) + (1,) * (values.ndim - 2) + (half_dim,)
    cosine = jnp.cos(angles).reshape(shape)
    sine = jnp.sin(angles).reshape(shape)
    first_half = values[..., :half_dim]
    second_half = values[..., half_dim:]
    return jnp.concatenate([first_half * cosine - second_half * sine, second_half * cosine + first_half * sine], axis=-1)

def one_sequence(inputs, segment_row, pre_gain, w_qkv, w_out, post_gain):
    seq_len = inputs.shape[0]
    groups = Q_HEADS // KV_HEADS
    widened = inputs.astype(jnp.float32)
    normed = rms_scale(widened, pre_gain).astype(jnp.bfloat16)
    projected = jnp.dot(normed, w_qkv, preferred_element_type=jnp.float32)
    positions = jnp.arange(seq_len, dtype=jnp.int32)
    queries = rotary(projected[:, :Q_HEADS * HEAD].reshape(seq_len, KV_HEADS, groups, HEAD), positions)
    key_rows = rotary(projected[:, Q_HEADS * HEAD:(Q_HEADS + KV_HEADS) * HEAD].reshape(seq_len, KV_HEADS, HEAD), positions)
    value_rows = projected[:, (Q_HEADS + KV_HEADS) * HEAD:].reshape(seq_len, KV_HEADS, HEAD)
    query_full = barrier_round(queries)
    key_full = barrier_round(key_rows)
    value_full = barrier_round(value_rows)
    doc_numbers = jnp.arange(DOCS, dtype=jnp.int32)
    matches = segment_row[:, None] == doc_numbers[None, :]
    first_pos = lax.optimization_barrier(jnp.min(jnp.where(matches, positions[:, None], seq_len), axis=0)).astype(jnp.int32)
    starts = lax.optimization_barrier(jnp.sum(jnp.where(matches, first_pos[None, :], 0), axis=1)).astype(jnp.int32)
    key_pad = jnp.concatenate([jnp.zeros((WINDOW, KV_HEADS, HEAD), jnp.float32), key_full], axis=0)
    value_pad = jnp.concatenate([jnp.zeros((WINDOW, KV_HEADS, HEAD), jnp.float32), value_full], axis=0)
    scale = 1.0 / math.sqrt(HEAD)

    def block(index):
        qstart = (index * TOK_DEV).astype(jnp.int32)
        query_block = lax.dynamic_slice_in_dim(query_full, qstart, TOK_DEV, 0)
        key_block = lax.dynamic_slice_in_dim(key_pad, qstart, WINDOW + TOK_DEV, 0)
        value_block = lax.dynamic_slice_in_dim(value_pad, qstart, WINDOW + TOK_DEV, 0)
        start_block = lax.dynamic_slice_in_dim(starts, qstart, TOK_DEV, 0)
        query_pos = qstart + jnp.arange(TOK_DEV, dtype=jnp.int32)
        key_pos = qstart - WINDOW + jnp.arange(WINDOW + TOK_DEV, dtype=jnp.int32)
        scores = jnp.einsum('qhgd,khd->qhgk', query_block, key_block) * scale
        capped = CAP * jnp.tanh(scores / CAP)
        allowed = (key_pos[None, :] <= query_pos[:, None]) & (query_pos[:, None] - key_pos[None, :] < WINDOW) & (key_pos[None, :] >= start_block[:, None])
        weights = jnp.where(allowed[:, None, None, :], jnp.exp(capped), 0.0)
        totals = lax.optimization_barrier(jnp.sum(weights, axis=-1))
        mixed = jnp.einsum('qhgk,khd->qhgd', barrier_round(weights), value_block)
        return (mixed / totals[..., None]).astype(jnp.bfloat16).reshape(TOK_DEV, Q_HEADS * HEAD)
    attended = lax.map(block, jnp.arange(seq_len // TOK_DEV, dtype=jnp.int32)).reshape(seq_len, Q_HEADS * HEAD)
    branch = jnp.dot(attended, w_out, preferred_element_type=jnp.float32)
    return (widened + rms_scale(branch, post_gain)).astype(jnp.bfloat16)

def reference(hidden_in, segment_ids, pre_gain, w_qkv, w_out, post_gain):
    results = []
    for row in range(BATCH):
        results.append(one_sequence(hidden_in[row], segment_ids[row], pre_gain, w_qkv, w_out, post_gain))
    return jnp.stack(results, axis=0)
```

```python
import functools
import math

import jax
import jax.numpy as jnp
import numpy as np
from jax import lax
from jax.experimental import pallas as pl
from jax.experimental.pallas import tpu as pltpu
from jax.sharding import PartitionSpec as P

Q_HEADS = 4
KV_HEADS = 2
HEAD = 256
WINDOW = 4096
DOCS = 16


EPS = 1e-06
CAP = 50.0


def from_behind(block, axis, distance):
    devices = range(lax.axis_size(axis))
    route = [(i - distance, i) for i in devices if i - distance in devices]
    return lax.ppermute(block, axis, route)


def rms_scale(values, gain):
    return values * lax.rsqrt(jnp.mean(values * values, axis=-1, keepdims=True) + EPS) * gain


def rotary(values, positions, leading):
    head_size = values.shape[-1]
    half_dim = head_size // 2
    inverse = 1.0 / 10000.0 ** (jnp.arange(half_dim, dtype=jnp.float32) * 2.0 / head_size)
    angles = positions.astype(jnp.float32)[:, None] * inverse[None, :]
    shape = (
        (1,) * leading + (positions.shape[0],) + (1,) * (values.ndim - 2 - leading) + (half_dim,)
    )
    cosine = jnp.cos(angles).reshape(shape)
    sine = jnp.sin(angles).reshape(shape)
    first_half = values[..., :half_dim]
    second_half = values[..., half_dim:]
    return jnp.concatenate(
        [first_half * cosine - second_half * sine, second_half * cosine + first_half * sine],
        axis=-1,
    )


def plain_layer(hidden_in, segment_ids, pre_gain, w_qkv, w_out, post_gain):
    tok_rows = hidden_in.shape[1]
    seq_count = lax.axis_size("seq")
    seq_index = lax.axis_index("seq")
    groups = Q_HEADS // KV_HEADS
    doc_most = min(WINDOW, seq_count * tok_rows // 8)
    hops = min(-(-(doc_most - 1) // tok_rows), seq_count - 1)
    positions = seq_index * tok_rows + jnp.arange(tok_rows, dtype=jnp.int32)
    own_ids = segment_ids[0]
    id_blocks = [from_behind(own_ids, "seq", d) for d in range(hops, 0, -1)] + [own_ids]
    widened = hidden_in[0].astype(jnp.float32)
    normed = rms_scale(widened, pre_gain).astype(jnp.bfloat16)
    projected = jnp.dot(
        normed,
        lax.all_gather(w_qkv, "seq", axis=0, tiled=True),
        preferred_element_type=jnp.float32,
    )
    queries = rotary(
        projected[:, : Q_HEADS * HEAD].reshape(tok_rows, KV_HEADS, groups, HEAD), positions, 0
    ).astype(jnp.bfloat16)
    key_rows = rotary(
        projected[:, Q_HEADS * HEAD : (Q_HEADS + KV_HEADS) * HEAD].reshape(
            tok_rows, KV_HEADS, HEAD
        ),
        positions,
        0,
    ).astype(jnp.bfloat16)
    value_rows = projected[:, (Q_HEADS + KV_HEADS) * HEAD :].astype(jnp.bfloat16)
    both = jnp.concatenate([key_rows.reshape(tok_rows, KV_HEADS * HEAD), value_rows], axis=1)
    blocks = [from_behind(both, "seq", d) for d in range(hops, 0, -1)] + [both]
    kv = jnp.concatenate(blocks, axis=0).reshape(-1, 2, KV_HEADS, HEAD)
    ids = jnp.concatenate(id_blocks, axis=0)
    key_pos = (seq_index - hops) * tok_rows + jnp.arange((hops + 1) * tok_rows, dtype=jnp.int32)
    allowed = (
        (key_pos[None, :] >= 0)
        & (key_pos[None, :] <= positions[:, None])
        & (positions[:, None] - key_pos[None, :] < WINDOW)
        & (ids[None, :] == own_ids[:, None])
    )
    scores = jnp.einsum(
        "qhgd,khd->hgqk", queries, kv[:, 0], preferred_element_type=jnp.float32
    ) * (1.0 / math.sqrt(HEAD))
    capped = CAP * jnp.tanh(scores / CAP)
    weights = jnp.where(allowed[None, None], jnp.exp(capped), 0.0)
    totals = jnp.sum(weights, axis=-1)
    mixed = jnp.einsum(
        "hgqk,khd->hgqd", weights.astype(jnp.bfloat16), kv[:, 1], preferred_element_type=jnp.float32
    )
    attended = (mixed / totals[..., None]).astype(jnp.bfloat16)
    attended = attended.transpose(2, 0, 1, 3).reshape(tok_rows, Q_HEADS * HEAD)
    branch = jnp.dot(
        attended,
        lax.all_gather(w_out, "seq", axis=0, tiled=True),
        preferred_element_type=jnp.float32,
    )
    return (widened + rms_scale(branch, post_gain)).astype(jnp.bfloat16)[None]


def split_rows(rows):
    first = (rows // 16 + 1) // 2 * 16
    return ((0, first), (first, rows - first))


class Ring:
    def __init__(self, place, classes, own_spot, full_spot, send_sems, recv_sems):
        self.place, self.classes = place, classes
        self.own_spot, self.full_spot = own_spot, full_spot
        self.send_sems, self.recv_sems = send_sems, recv_sems
        self.far = place["chips"] // 2
        self.near = place["chips"] - 1 - self.far
        self.relays = len(classes) * 2 * self.far
        self.extra = 2 * self.relays
        self.started = []

    def reach(self, piece, way):
        return self.far if self.classes[piece] == way else self.near

    def slot(self, piece, way, hop):
        return (piece * 2 + way) * self.far + hop - 1

    def origin(self, way, hop):
        return self.place["chip_at"](self.place["ring"] + (hop if way else -hop))

    def spot(self, piece, way, hop, core):
        return self.full_spot(piece, self.origin(way, hop) * 2 + core)

    def copy(self, source, target, slot, device):
        return pltpu.make_async_remote_copy(
            src_ref=source,
            dst_ref=target,
            send_sem=self.send_sems.at[slot],
            recv_sem=self.recv_sems.at[slot],
            device_id=device,
            device_id_type=pl.DeviceIdType.MESH,
        )

    def send(self, source, target, slot, device):
        moving = self.copy(source, target, slot, device)
        moving.start()
        self.started.append(moving)

    def arrived(self, spot, slot):
        self.copy(spot, spot, slot, self.place["sibling"]).wait_recv()

    def first(self, pieces):
        for piece in pieces:
            for way in (0, 1):
                self.send(
                    self.own_spot(piece),
                    self.full_spot(piece, self.place["seq"]),
                    self.slot(piece, way, 1),
                    self.place["onward"][way],
                )

    def step(self, hop, pieces, then=None):
        place = self.place
        for piece in pieces:
            for way in (0, 1):
                if hop > self.reach(piece, way):
                    continue
                spot = self.spot(piece, way, hop, place["core"])
                slot = self.slot(piece, way, hop)
                self.arrived(spot, slot)
                if hop < self.reach(piece, way):
                    self.send(spot, spot, slot + 1, place["onward"][way])
                if then is not None:
                    then(piece, way, hop, spot)
                self.send(spot, spot, self.relays + slot, place["sibling"])

    def relayed(self, pieces):
        other = 1 - self.place["core"]
        for piece in pieces:
            for way in (0, 1):
                for hop in range(1, self.reach(piece, way) + 1):
                    self.arrived(
                        self.spot(piece, way, hop, other), self.relays + self.slot(piece, way, hop)
                    )

    def drain(self):
        for moving in self.started:
            moving.wait_send()


def layer_kernel(
    chips, hid, ids, inverse_in, pre_in, w_qkv, w_out, post_in, result,
    ids0, inverse, pre, post, out, wq, wo, own, guest, nrm, qry, kv, kv1, kv2, ids1, far0, far1, near0, near1,
    cos, sin, acc, tot, att, attx, branch,
    q_send, q_recv, o_send, o_recv, s_send, s_recv, local_sem,
):
    seq, x = lax.axis_index("seq"), lax.axis_index("batch")
    chip, core = seq // 2, seq % 2
    half = chips // 2
    layer, side = chip // 2, chip % 2
    ring = (1 - side) * layer + side * (chips - 1 - layer)

    def chip_at(position):
        position = (position + chips) % chips
        far = position // half
        return (1 - far) * 2 * position + far * (2 * (chips - 1 - position) + 1)

    def at(device_chip, device_core, batch):
        return {"seq": device_chip * 2 + device_core, "batch": batch}

    up, down = at(chip_at(ring + 1), core, x), at(chip_at(ring - 1), core, x)
    sibling, across = at(chip, 1 - core, x), at(chip, core, 1 - x)
    after = at((chip + 1) % chips, core, x)
    before = at((chip + chips - 1) % chips, core, x)
    place = dict(
        chips=chips, seq=seq, core=core, ring=ring, chip_at=chip_at, sibling=sibling,
        onward=(up, down),
    )
    tokens, width = own.shape
    rows_q, rows_o = w_qkv.shape[0], w_out.shape[0]
    group = Q_HEADS // KV_HEADS
    third_width = width // 6

    def local(source, target, slot):
        moving = pltpu.make_async_copy(source, target, local_sem.at[slot])
        moving.start()
        return moving

    column_at = [
        (Q_HEADS + x) * HEAD, (Q_HEADS + KV_HEADS + x) * HEAD
    ] + [(group * x + head) * HEAD for head in range(group)]

    def columns_of(kind):
        return pl.ds(pl.multiple_of(column_at[kind], HEAD), HEAD)

    kinds = len(column_at)
    q_pieces = [(kind, start, count) for kind in range(kinds) for start, count in split_rows(rows_q)]

    def q_own(piece):
        kind, start, count = q_pieces[piece]
        return w_qkv.at[pl.ds(start, count), columns_of(kind)]

    def q_full(piece, device):
        kind, start, count = q_pieces[piece]
        return wq.at[kind, pl.ds(pl.multiple_of(device * rows_q + start, 16), count), :]

    def q_rows(kind, device):
        return wq.at[kind, pl.ds(pl.multiple_of(device * rows_q, 16), rows_q), :]

    def o_columns(third, unit):
        return pl.ds(pl.multiple_of((third * 2 + unit) * third_width, 128), third_width)

    def o_rows(device):
        return pl.ds(pl.multiple_of(device * rows_o, 16), rows_o)

    o_thirds = (2 * x, 1)

    def o_own(piece):
        return w_out.at[:, o_columns(o_thirds[piece % 2], piece // 2)]

    def o_full(piece, device):
        return wo.at[o_rows(device), o_columns(o_thirds[piece % 2], piece // 2)]

    gather_q = Ring(place, [kind % 2 for kind, _, _ in q_pieces], q_own, q_full, q_send, q_recv)
    gather_o = Ring(place, [0, 1, 0, 1], o_own, o_full, o_send, o_recv)

    ids_copy = local(ids, ids0, kinds + 2)
    own_copies = [local(hid, own, 0)]
    table_copies = [
        local(source, target, kinds + 3 + index)
        for index, (source, target) in enumerate(((inverse_in, inverse), (pre_in, pre), (post_in, post)))
    ]
    for kind in range(kinds):
        own_copies.append(local(w_qkv.at[:, columns_of(kind)], q_rows(kind, seq), kind + 1))
    own_copies.append(local(w_out, wo.at[o_rows(seq), :], kinds + 1))

    met = [sibling, across, up, down, after, before]
    barrier = pltpu.get_barrier_semaphore()
    for other in met:
        pl.semaphore_signal(barrier, 1, device_id=other, device_id_type=pl.DeviceIdType.MESH)
    ids_copy.wait()
    pl.semaphore_wait(barrier, len(met))

    def small(source, target, slot, device):
        return pltpu.make_async_remote_copy(
            src_ref=source, dst_ref=target, send_sem=s_send.at[slot], recv_sem=s_recv.at[slot],
            device_id=device, device_id_type=pl.DeviceIdType.MESH,
        )

    early = [piece for piece in range(len(q_pieces)) if q_pieces[piece][0] < 2]
    late = [piece for piece in range(len(q_pieces)) if q_pieces[piece][0] >= 2]
    crossers, others = (0, 2), (1, 3)
    o_pieces = crossers + others
    ids_across = small(ids0, ids1, 0, across)
    ids_across.start()
    ids_after = [small(ids0, far0, 1, after), small(ids1, far1, 2, after)]
    ids_after[0].start()
    gather_q.first(early)
    portion = tokens // 4
    guests = []
    for index in range(4):
        part = pl.ds(index * portion, portion)
        guests.append(small(hid.at[part, :], guest.at[part, :], 10 + index, across))
        guests[-1].start()
    for kind in range(kinds):
        gather_q.send(
            w_qkv.at[:, columns_of(kind)], q_rows(kind, seq), gather_q.extra + kind, sibling
        )
    gather_o.send(w_out, wo.at[o_rows(seq), :], gather_o.extra, sibling)

    strip = 16

    def normalize(source, base, start, count):
        @pl.loop(0, count // strip, unroll=2)
        def _(index):
            at_row = pl.multiple_of(start + index * strip, strip)
            values = source[pl.ds(at_row, strip), :].astype(jnp.float32)
            nrm[pl.ds(pl.multiple_of(base + at_row, strip), strip), :] = rms_scale(
                values, pre[...]
            ).astype(jnp.bfloat16)

    def pass_on(mine, far, near, slot):
        @pl.when(core == 0)
        def _():
            small(mine, near, slot, sibling).start()

        @pl.when(core == 1)
        def _():
            small(far, near, slot, sibling).start()

    def ids_near():
        ids_after[0].wait()
        ids_after[1].wait()
        pass_on(ids0, far0, near0, 3)
        pass_on(ids1, far1, near1, 4)

    def slot_rows(slot):
        return pl.ds(slot * tokens, tokens)

    def project(slot, kind):
        return jnp.dot(nrm[slot_rows(slot), :], wq[kind], preferred_element_type=jnp.float32)

    def turned(values):
        a, b = values[:, : HEAD // 2], values[:, HEAD // 2 :]
        c, s = cos[...], sin[...]
        return jnp.concatenate([a * c - b * s, b * c + a * s], axis=1).astype(jnp.bfloat16)

    def kv_moving(slot):
        return small(kv.at[slot_rows(slot), :], kv2.at[slot_rows(slot), :], 5 + slot, after)

    def make_kv(slot):
        kv[slot_rows(slot), :HEAD] = turned(project(slot, 0))
        kv[slot_rows(slot), HEAD:] = project(slot, 1).astype(jnp.bfloat16)

        @pl.when(chip < chips - 1)
        def _():
            kv_moving(slot).start()

    def take_kv(slot):
        @pl.when(chip > 0)
        def _():
            kv_moving(slot).wait_recv()

        rows = slot_rows(slot)
        pass_on(kv.at[rows, :], kv2.at[rows, :], kv1.at[rows, :], 7 + slot)

    def take_near(slot):
        rows = slot_rows(slot)
        small(kv.at[rows, :], kv1.at[rows, :], 7 + slot, sibling).wait()

    def make_queries(slot):
        for head in range(group):
            qry[slot_rows(slot), head * HEAD : (head + 1) * HEAD] = turned(project(slot, 2 + head))

    def take_guest(index):
        guests[index].wait()
        normalize(guest, tokens, index * portion, portion)

    def shared(kind):
        gather_q.arrived(q_rows(kind, seq + 1 - 2 * core), gather_q.extra + kind)

    def over(piece, way, hop, spot):
        if piece % 2 == 0:
            gather_o.send(spot, spot, crossing(piece, way, hop), across)

    def crossing(piece, way, hop):
        return gather_o.extra + 1 + ((piece // 2) * 2 + way) * gather_o.far + hop - 1

    crossings = 4 * gather_o.far

    def crossed_spot(piece, way, hop, on_core):
        device = gather_o.origin(way, hop) * 2 + on_core
        return wo.at[o_rows(device), o_columns(2 - 2 * x, piece // 2)]

    def crossed(hop, pieces):
        for piece in pieces:
            for way in (0, 1):
                if piece % 2 or hop > gather_o.reach(piece, way):
                    continue
                spot = crossed_spot(piece, way, hop, core)
                gather_o.arrived(spot, crossing(piece, way, hop))
                gather_o.send(spot, spot, crossings + crossing(piece, way, hop), sibling)

    def crossed_relayed(pieces):
        for piece in pieces:
            for way in (0, 1):
                if piece % 2:
                    continue
                for hop in range(1, gather_o.reach(piece, way) + 1):
                    gather_o.arrived(
                        crossed_spot(piece, way, hop, 1 - core),
                        crossings + crossing(piece, way, hop),
                    )

    row = lax.broadcasted_iota(jnp.int32, (tokens, tokens), 0)
    column = lax.broadcasted_iota(jnp.int32, (tokens, tokens), 1)

    def as_column(ids):
        spread = jnp.broadcast_to(ids[...], (tokens, tokens))
        return jnp.sum(jnp.where(row == column, spread, 0), axis=1, keepdims=True)

    def block(slot, head, source, allowed, first):
        rows = slot_rows(slot)
        columns = slice(head * HEAD, (head + 1) * HEAD)
        lanes = slice(head * 128, (head + 1) * 128)
        scores = lax.dot_general(
            qry[rows, columns], source[rows, :HEAD], (((1,), (1,)), ((), ())),
            preferred_element_type=jnp.float32,
        )
        bent = jnp.tanh(scores * (1.0 / (math.sqrt(HEAD) * CAP)))
        weights = jnp.where(allowed, jnp.exp2(bent * (CAP * math.log2(math.e))), 0.0)
        total = jnp.broadcast_to(jnp.sum(weights, axis=1, keepdims=True), (tokens, 128))
        mixed = jnp.dot(
            weights.astype(jnp.bfloat16), source[rows, HEAD:], preferred_element_type=jnp.float32
        )
        if first:
            acc[rows, columns] = mixed
            tot[rows, lanes] = total
        else:
            acc[rows, columns] += mixed
            tot[rows, lanes] += total

    def blocks(slot, source, allowed, first):
        for head in range(group):
            block(slot, head, source, allowed, first)

    def own_block(slot):
        ids = (ids0, ids1)[slot]
        blocks(slot, kv, (column <= row) & (as_column(ids) == ids[...]), True)

    def far_block(slot):
        ids = as_column((ids0, ids1)[slot])
        blocks(slot, kv2, (ids == (far0, far1)[slot][...]) & (row + seq >= row + 2), False)

    def near_block(slot):
        ids = as_column((ids0, ids1)[slot])
        blocks(slot, kv1, (ids == (near0, near1)[slot][...]) & (row + seq >= row + 1), False)
        rows = slot_rows(slot)
        for head in range(group):
            columns = slice(head * HEAD, (head + 1) * HEAD)
            att[rows, columns] = (acc[rows, columns] / tot[rows, head * 128 : head * 128 + 1]).astype(
                jnp.bfloat16
            )

    own_copies[0].wait()
    for moving in table_copies:
        moving.wait()
    normalize(own, 0, 0, tokens)
    gather_q.step(1, early)
    ids_across.wait()
    ids_after[1].start()
    positions = seq * tokens + lax.broadcasted_iota(jnp.int32, cos.shape, 0)
    angles = positions.astype(jnp.float32) * inverse[...]
    cos[...] = jnp.cos(angles)
    sin[...] = jnp.sin(angles)

    @pl.when(chip == 0)
    def _():
        kv2[...] = jnp.zeros_like(kv2)

    for hop in range(2, gather_q.near + 1):
        gather_q.step(hop, early)
    gather_q.first(late)
    for hop in range(gather_q.near + 1, gather_q.far + 1):
        gather_q.step(hop, early)
    gather_q.step(1, late)
    gather_o.first(crossers)
    for moving in own_copies[1:]:
        moving.wait()
    gather_q.relayed(early)
    shared(0)
    shared(1)
    make_kv(0)
    gather_q.step(2, late)
    take_guest(0)
    gather_o.step(1, crossers, over)
    take_guest(1)
    for hop in range(3, gather_q.near + 1):
        gather_q.step(hop, late)
    gather_o.step(2, crossers, over)
    take_guest(2)
    take_guest(3)
    make_kv(1)
    gather_o.first(others)
    ids_near()
    for hop in range(gather_q.near + 1, gather_q.far + 1):
        gather_q.step(hop, late)
    take_kv(0)
    for hop in range(3, gather_o.near + 1):
        gather_o.step(hop, crossers, over)
    gather_q.relayed(late)
    for kind in range(2, kinds):
        shared(kind)
    make_queries(0)
    make_queries(1)
    own_block(0)
    own_block(1)
    gather_o.step(1, others)
    small(ids0, near0, 3, sibling).wait()
    small(ids1, near1, 4, sibling).wait()
    far_block(0)
    take_near(0)
    near_block(0)
    for hop in range(gather_o.near + 1, gather_o.far + 1):
        gather_o.step(hop, crossers, over)
    gather_o.step(2, others)
    take_kv(1)
    far_block(1)
    take_near(1)
    near_block(1)
    att_moving = small(att.at[slot_rows(1), :], attx, 9, across)
    att_moving.start()
    for hop in range(3, gather_o.far + 1):
        gather_o.step(hop, others)
    for hop in range(1, gather_o.far + 1):
        crossed(hop, o_pieces)
    gather_o.relayed(o_pieces)
    crossed_relayed(o_pieces)
    gather_o.arrived(wo.at[o_rows(seq + 1 - 2 * core), :], gather_o.extra)
    mine_at = pl.ds(pl.multiple_of(x * group * HEAD, HEAD), group * HEAD)
    theirs_at = pl.ds(pl.multiple_of((1 - x) * group * HEAD, HEAD), group * HEAD)
    att_moving.wait()
    for start in range(0, width, 256):
        chunk = slice(start, start + 256)
        branch[:, chunk] = jnp.dot(
            att[slot_rows(0), :], wo[mine_at, chunk], preferred_element_type=jnp.float32
        ) + jnp.dot(attx[...], wo[theirs_at, chunk], preferred_element_type=jnp.float32)

    leaving = []
    for index in range(4):
        @pl.loop(index * portion // strip, (index + 1) * portion // strip, unroll=2)
        def _(step):
            rows = pl.ds(pl.multiple_of(step * strip, strip), strip)
            scaled = rms_scale(branch[rows, :], post[...])
            out[rows, :] = (own[rows, :].astype(jnp.float32) + scaled).astype(jnp.bfloat16)

        part = pl.ds(index * portion, portion)
        leaving.append(local(out.at[part, :], result.at[part, :], kinds + 6 + index))

    for slot in range(2):
        @pl.when(chip < chips - 1)
        def _():
            kv_moving(slot).wait_send()
    gather_q.drain()
    gather_o.drain()
    for moving in leaving:
        moving.wait()


def paired_layer(hidden_in, segment_ids, pre_gain, w_qkv, w_out, post_gain):
    tokens, width = hidden_in.shape[1:]
    chips = lax.axis_size("seq") // 2
    bf16, f32 = jnp.bfloat16, jnp.float32
    steps = np.arange(HEAD // 2, dtype=np.float32) * np.float32(2.0 / HEAD)
    inverse = np.float32(1.0) / np.float32(10000.0) ** steps
    vmem, dma = pltpu.VMEM, pltpu.SemaphoreType.DMA
    group = Q_HEADS // KV_HEADS
    heads = group * HEAD
    far = chips // 2
    q_sems = 2 * 2 * (2 + group) * 2 * far + 2 + group
    o_sems = 2 * 4 * 2 * far + 1 + 2 * 4 * far
    anywhere = pl.BlockSpec(memory_space=pl.ANY)
    result = pl.pallas_call(
        functools.partial(layer_kernel, chips),
        out_shape=jax.ShapeDtypeStruct((tokens, width), bf16),
        in_specs=[anywhere] * 7,
        out_specs=anywhere,
        scratch_shapes=[
            vmem((1, tokens), jnp.int32),
            vmem((1, HEAD // 2), f32),
            vmem((width,), f32),
            vmem((width,), f32),
            vmem((tokens, width), bf16),
            vmem((2 + group, width, HEAD), bf16),
            vmem((w_out.shape[0] * chips * 2, width), bf16),
            vmem((tokens, width), bf16),
            vmem((tokens, width), bf16),
            vmem((2 * tokens, width), bf16),
            vmem((2 * tokens, heads), bf16),
            vmem((2 * tokens, 2 * HEAD), bf16),
            vmem((2 * tokens, 2 * HEAD), bf16),
            vmem((2 * tokens, 2 * HEAD), bf16),
            vmem((1, tokens), jnp.int32),
            vmem((1, tokens), jnp.int32),
            vmem((1, tokens), jnp.int32),
            vmem((1, tokens), jnp.int32),
            vmem((1, tokens), jnp.int32),
            vmem((tokens, HEAD // 2), f32),
            vmem((tokens, HEAD // 2), f32),
            vmem((2 * tokens, heads), f32),
            vmem((2 * tokens, group * 128), f32),
            vmem((2 * tokens, heads), bf16),
            vmem((tokens, heads), bf16),
            vmem((tokens, width), f32),
            dma((q_sems,)),
            dma((q_sems,)),
            dma((o_sems,)),
            dma((o_sems,)),
            dma((14,)),
            dma((14,)),
            dma((12 + group,)),
        ],
        compiler_params=pltpu.CompilerParams(
            collective_id=0, has_side_effects=True, vmem_limit_bytes=58 * 1024 * 1024
        ),
    )(
        hidden_in[0],
        segment_ids,
        jnp.asarray(inverse)[None, :],
        pre_gain,
        w_qkv,
        w_out,
        post_gain,
    )
    return result[None]


def per_device(hidden_in, segment_ids, pre_gain, w_qkv, w_out, post_gain):
    tokens, width = hidden_in.shape[1:]
    seq_count = lax.axis_size("seq")
    doc_most = min(WINDOW, seq_count * tokens // 8)
    whole_tiles = w_qkv.shape[0] % 16 == 0 and w_out.shape[0] % 16 == 0 and width % 768 == 0
    two_hops = doc_most - 1 <= 2 * tokens and 3 * tokens <= WINDOW
    small_ring = seq_count % 4 == 0 and seq_count > 12
    if whole_tiles and two_hops and small_ring and lax.axis_size("batch") == 2 and KV_HEADS == 2:
        layer = paired_layer
    else:
        layer = plain_layer
    return layer(hidden_in, segment_ids, pre_gain, w_qkv, w_out, post_gain)


def solution(mesh):
    placed = (P("batch", "seq", None), P("batch", "seq"), P(), P("seq", None), P("seq", None), P())
    return jax.shard_map(
        per_device, mesh=mesh, in_specs=placed, out_specs=P("batch", "seq", None), check_vma=False
    )
```

```python
import functools
import math

import jax
import jax.numpy as jnp
import numpy as np
from jax import lax
from jax.experimental import pallas as pl
from jax.experimental.pallas import tpu as pltpu
from jax.sharding import PartitionSpec as P

Q_HEADS = 4
KV_HEADS = 2
HEAD = 256
WINDOW = 4096
DOCS = 16


EPS = 1e-06
CAP = 50.0


def from_behind(block, axis, distance):
    devices = range(lax.axis_size(axis))
    route = [(i - distance, i) for i in devices if i - distance in devices]
    return lax.ppermute(block, axis, route)


def rms_scale(values, gain):
    return values * lax.rsqrt(jnp.mean(values * values, axis=-1, keepdims=True) + EPS) * gain


def rotary(values, positions, leading):
    head_size = values.shape[-1]
    half_dim = head_size // 2
    inverse = 1.0 / 10000.0 ** (jnp.arange(half_dim, dtype=jnp.float32) * 2.0 / head_size)
    angles = positions.astype(jnp.float32)[:, None] * inverse[None, :]
    shape = (
        (1,) * leading + (positions.shape[0],) + (1,) * (values.ndim - 2 - leading) + (half_dim,)
    )
    cosine = jnp.cos(angles).reshape(shape)
    sine = jnp.sin(angles).reshape(shape)
    first_half = values[..., :half_dim]
    second_half = values[..., half_dim:]
    return jnp.concatenate(
        [first_half * cosine - second_half * sine, second_half * cosine + first_half * sine],
        axis=-1,
    )


def plain_layer(hidden_in, segment_ids, pre_gain, w_qkv, w_out, post_gain):
    tok_rows = hidden_in.shape[1]
    seq_count = lax.axis_size("seq")
    seq_index = lax.axis_index("seq")
    groups = Q_HEADS // KV_HEADS
    doc_most = min(WINDOW, seq_count * tok_rows // 8)
    hops = min(-(-(doc_most - 1) // tok_rows), seq_count - 1)
    positions = seq_index * tok_rows + jnp.arange(tok_rows, dtype=jnp.int32)
    own_ids = segment_ids[0]
    id_blocks = [from_behind(own_ids, "seq", d) for d in range(hops, 0, -1)] + [own_ids]
    widened = hidden_in[0].astype(jnp.float32)
    normed = rms_scale(widened, pre_gain).astype(jnp.bfloat16)
    projected = jnp.dot(
        normed,
        lax.all_gather(w_qkv, "seq", axis=0, tiled=True),
        preferred_element_type=jnp.float32,
    )
    queries = rotary(
        projected[:, : Q_HEADS * HEAD].reshape(tok_rows, KV_HEADS, groups, HEAD), positions, 0
    ).astype(jnp.bfloat16)
    key_rows = rotary(
        projected[:, Q_HEADS * HEAD : (Q_HEADS + KV_HEADS) * HEAD].reshape(
            tok_rows, KV_HEADS, HEAD
        ),
        positions,
        0,
    ).astype(jnp.bfloat16)
    value_rows = projected[:, (Q_HEADS + KV_HEADS) * HEAD :].astype(jnp.bfloat16)
    both = jnp.concatenate([key_rows.reshape(tok_rows, KV_HEADS * HEAD), value_rows], axis=1)
    blocks = [from_behind(both, "seq", d) for d in range(hops, 0, -1)] + [both]
    kv = jnp.concatenate(blocks, axis=0).reshape(-1, 2, KV_HEADS, HEAD)
    ids = jnp.concatenate(id_blocks, axis=0)
    key_pos = (seq_index - hops) * tok_rows + jnp.arange((hops + 1) * tok_rows, dtype=jnp.int32)
    allowed = (
        (key_pos[None, :] >= 0)
        & (key_pos[None, :] <= positions[:, None])
        & (positions[:, None] - key_pos[None, :] < WINDOW)
        & (ids[None, :] == own_ids[:, None])
    )
    scores = jnp.einsum(
        "qhgd,khd->hgqk", queries, kv[:, 0], preferred_element_type=jnp.float32
    ) * (1.0 / math.sqrt(HEAD))
    capped = CAP * jnp.tanh(scores / CAP)
    weights = jnp.where(allowed[None, None], jnp.exp(capped), 0.0)
    totals = jnp.sum(weights, axis=-1)
    mixed = jnp.einsum(
        "hgqk,khd->hgqd", weights.astype(jnp.bfloat16), kv[:, 1], preferred_element_type=jnp.float32
    )
    attended = (mixed / totals[..., None]).astype(jnp.bfloat16)
    attended = attended.transpose(2, 0, 1, 3).reshape(tok_rows, Q_HEADS * HEAD)
    branch = jnp.dot(
        attended,
        lax.all_gather(w_out, "seq", axis=0, tiled=True),
        preferred_element_type=jnp.float32,
    )
    return (widened + rms_scale(branch, post_gain)).astype(jnp.bfloat16)[None]


def split_rows(rows):
    first = (rows // 16 + 1) // 2 * 16
    return ((0, first), (first, rows - first))


class Ring:
    def __init__(self, place, classes, own_spot, full_spot, send_sem, recv_sems):
        self.place, self.classes = place, classes
        self.own_spot, self.full_spot = own_spot, full_spot
        self.send_sem, self.recv_sems = send_sem, recv_sems
        self.far = place["chips"] // 2
        self.near = place["chips"] - 1 - self.far
        self.extra = len(classes) * (self.far + self.near)

    def reach(self, piece, way):
        return self.far if self.classes[piece] == way else self.near

    def slot(self, piece, way, hop):
        onset = 0 if self.classes[piece] == way else self.far
        return piece * (self.far + self.near) + onset + hop - 1

    def origin(self, way, hop):
        return self.place["chip_at"](self.place["ring"] + (hop if way else -hop))

    def spot(self, piece, way, hop):
        return self.full_spot(piece, self.origin(way, hop) * 2 + self.place["core"])

    def copy(self, source, target, slot, device):
        return pltpu.make_async_remote_copy(
            src_ref=source,
            dst_ref=target,
            send_sem=self.send_sem.at[0],
            recv_sem=self.recv_sems.at[slot],
            device_id=device,
            device_id_type=pl.DeviceIdType.MESH,
        )

    def send(self, source, target, slot, device):
        self.copy(source, target, slot, device).start()

    def arrived(self, spot, slot):
        self.copy(spot, spot, slot, self.place["sibling"]).wait_recv()

    def sent(self, as_much):
        self.copy(as_much, as_much, 0, self.place["sibling"]).wait_send()

    def first(self, pieces):
        for piece in pieces:
            for way in (0, 1):
                self.send(
                    self.own_spot(piece),
                    self.full_spot(piece, self.place["seq"]),
                    self.slot(piece, way, 1),
                    self.place["onward"][way],
                )

    def step(self, hop, pieces, relay_slot, then=None):
        place = self.place
        for piece in pieces:
            for way in (0, 1):
                if hop > self.reach(piece, way):
                    continue
                spot = self.spot(piece, way, hop)
                slot = self.slot(piece, way, hop)
                self.arrived(spot, slot)
                if hop < self.reach(piece, way):
                    self.send(spot, spot, slot + 1, place["onward"][way])
                if then is not None:
                    then(piece, way, hop, spot)
                self.send(spot, spot, relay_slot, place["sibling"])


def layer_kernel(
    chips, hid, ids, inverse_in, pre_in, w_qkv, w_out, own, branch,
    ids0, inverse, pre, wq, wo, guest, nrm, qry, kv, kv1, kv2, ids1, far0, far1, near0, near1,
    cos, sin, acc, tot, att, attx,
    q_send, q_recv, o_send, o_recv, s_send, s_recv, local_sem,
):
    seq, x = lax.axis_index("seq"), lax.axis_index("batch")
    chip, core = seq // 2, seq % 2
    half = chips // 2
    layer, side = chip // 2, chip % 2
    ring = (1 - side) * layer + side * (chips - 1 - layer)

    def chip_at(position):
        position = (position + chips) % chips
        far = position // half
        return (1 - far) * 2 * position + far * (2 * (chips - 1 - position) + 1)

    def at(device_chip, device_core, batch):
        return {"seq": device_chip * 2 + device_core, "batch": batch}

    up, down = at(chip_at(ring + 1), core, x), at(chip_at(ring - 1), core, x)
    sibling, across = at(chip, 1 - core, x), at(chip, core, 1 - x)
    after = at((chip + 1) % chips, core, x)
    before = at((chip + chips - 1) % chips, core, x)
    place = dict(
        chips=chips, seq=seq, core=core, ring=ring, chip_at=chip_at, sibling=sibling,
        onward=(up, down),
    )
    tokens, width = own.shape
    rows_q, rows_o = w_qkv.shape[0], w_out.shape[0]
    group = Q_HEADS // KV_HEADS
    third_width = width // 6

    def local(source, target, slot):
        moving = pltpu.make_async_copy(source, target, local_sem.at[slot])
        moving.start()
        return moving

    column_at = [
        (Q_HEADS + x) * HEAD, (Q_HEADS + KV_HEADS + x) * HEAD
    ] + [(group * x + head) * HEAD for head in range(group)]

    def columns_of(kind):
        return pl.ds(pl.multiple_of(column_at[kind], HEAD), HEAD)

    kinds = len(column_at)
    q_pieces = [(kind, start, count) for kind in range(kinds) for start, count in split_rows(rows_q)]

    def q_own(piece):
        kind, start, count = q_pieces[piece]
        return w_qkv.at[pl.ds(start, count), columns_of(kind)]

    def q_full(piece, device):
        kind, start, count = q_pieces[piece]
        return wq.at[kind, pl.ds(pl.multiple_of(device * rows_q + start, 16), count), :]

    def q_rows(kind, device):
        return wq.at[kind, pl.ds(pl.multiple_of(device * rows_q, 16), rows_q), :]

    def o_columns(third, unit):
        return pl.ds(pl.multiple_of((third * 2 + unit) * third_width, 128), third_width)

    def o_rows(device):
        return pl.ds(pl.multiple_of(device * rows_o, 16), rows_o)

    o_thirds = (2 * x, 1)

    def o_own(piece):
        return w_out.at[:, o_columns(o_thirds[piece % 2], piece // 2)]

    def o_full(piece, device):
        return wo.at[o_rows(device), o_columns(o_thirds[piece % 2], piece // 2)]

    gather_q = Ring(place, [kind % 2 for kind, _, _ in q_pieces], q_own, q_full, q_send, q_recv)
    gather_o = Ring(place, [0, 1, 0, 1], o_own, o_full, o_send, o_recv)

    ids_copy = local(ids, ids0, kinds + 2)
    own_copies = [local(hid, own, 0)]
    table_copies = [
        local(source, target, kinds + 3 + index)
        for index, (source, target) in enumerate(((inverse_in, inverse), (pre_in, pre)))
    ]
    for kind in range(kinds):
        own_copies.append(local(w_qkv.at[:, columns_of(kind)], q_rows(kind, seq), kind + 1))
    own_copies.append(local(w_out, wo.at[o_rows(seq), :], kinds + 1))

    met = [sibling, across, up, down, after, before]
    barrier = pltpu.get_barrier_semaphore()
    for other in met:
        pl.semaphore_signal(barrier, 1, device_id=other, device_id_type=pl.DeviceIdType.MESH)
    ids_copy.wait()
    pl.semaphore_wait(barrier, len(met))

    def small(source, target, slot, device):
        return pltpu.make_async_remote_copy(
            src_ref=source, dst_ref=target, send_sem=s_send.at[slot], recv_sem=s_recv.at[slot],
            device_id=device, device_id_type=pl.DeviceIdType.MESH,
        )

    early = [piece for piece in range(len(q_pieces)) if q_pieces[piece][0] < 2]
    late = [piece for piece in range(len(q_pieces)) if q_pieces[piece][0] >= 2]
    crossers, others = (0, 2), (1, 3)
    early_relay, late_relay, o_relay = gather_q.extra, gather_q.extra + 1, gather_o.extra
    o_pieces = crossers + others
    ids_across = small(ids0, ids1, 0, across)
    ids_across.start()
    ids_after = [small(ids0, far0, 1, after), small(ids1, far1, 2, after)]
    ids_after[0].start()
    gather_q.first(early)
    portion = tokens // 4
    guests = []
    for index in range(4):
        part = pl.ds(index * portion, portion)
        guests.append(small(hid.at[part, :], guest.at[part, :], 10 + index, across))
        guests[-1].start()
    for kind in range(kinds):
        gather_q.send(
            w_qkv.at[:, columns_of(kind)], q_rows(kind, seq), early_relay + (kind >= 2), sibling
        )
    gather_o.send(w_out, wo.at[o_rows(seq), :], o_relay, sibling)

    strip = 16

    def normalize(source, base, start, count):
        @pl.loop(0, count // strip, unroll=2)
        def _(index):
            at_row = pl.multiple_of(start + index * strip, strip)
            values = source[pl.ds(at_row, strip), :].astype(jnp.float32)
            nrm[pl.ds(pl.multiple_of(base + at_row, strip), strip), :] = rms_scale(
                values, pre[...]
            ).astype(jnp.bfloat16)

    def pass_on(mine, far, near, slot):
        @pl.when(core == 0)
        def _():
            small(mine, near, slot, sibling).start()

        @pl.when(core == 1)
        def _():
            small(far, near, slot, sibling).start()

    def ids_near():
        ids_after[0].wait()
        ids_after[1].wait()
        pass_on(ids0, far0, near0, 3)
        pass_on(ids1, far1, near1, 4)

    def slot_rows(slot):
        return pl.ds(slot * tokens, tokens)

    def project(slot, kind):
        return jnp.dot(nrm[slot_rows(slot), :], wq[kind], preferred_element_type=jnp.float32)

    def turned(values):
        a, b = values[:, : HEAD // 2], values[:, HEAD // 2 :]
        c, s = cos[...], sin[...]
        return jnp.concatenate([a * c - b * s, b * c + a * s], axis=1).astype(jnp.bfloat16)

    def kv_moving(slot):
        return small(kv.at[slot_rows(slot), :], kv2.at[slot_rows(slot), :], 5 + slot, after)

    def make_kv(slot):
        kv[slot_rows(slot), :HEAD] = turned(project(slot, 0))
        kv[slot_rows(slot), HEAD:] = project(slot, 1).astype(jnp.bfloat16)

    def send_kv(slot):
        @pl.when(chip < chips - 1)
        def _():
            kv_moving(slot).start()

    def take_kv(slot):
        @pl.when(chip > 0)
        def _():
            kv_moving(slot).wait_recv()

        rows = slot_rows(slot)
        pass_on(kv.at[rows, :], kv2.at[rows, :], kv1.at[rows, :], 7 + slot)

    def take_near(slot):
        rows = slot_rows(slot)
        small(kv.at[rows, :], kv1.at[rows, :], 7 + slot, sibling).wait()

    def make_queries(slot):
        for head in range(group):
            qry[slot_rows(slot), head * HEAD : (head + 1) * HEAD] = turned(project(slot, 2 + head))

    def take_guest(index):
        guests[index].wait()
        normalize(guest, tokens, index * portion, portion)

    def over(piece, way, hop, spot):
        if piece in crossers:
            gather_o.send(spot, spot, crossing(piece, way, hop), across)

    def crossing(piece, way, hop):
        first = crossers.index(piece) - piece
        return o_relay + 1 + first * (chips - 1) + gather_o.slot(piece, way, hop)

    def crossed(hop, pieces):
        for piece in pieces:
            for way in (0, 1):
                if hop > gather_o.reach(piece, way):
                    continue
                device = gather_o.origin(way, hop) * 2 + core
                spot = wo.at[o_rows(device), o_columns(2 - 2 * x, piece // 2)]
                gather_o.arrived(spot, crossing(piece, way, hop))
                gather_o.send(spot, spot, o_relay, sibling)

    row = lax.broadcasted_iota(jnp.int32, (tokens, tokens), 0)
    column = lax.broadcasted_iota(jnp.int32, (tokens, tokens), 1)

    def as_column(ids):
        spread = jnp.broadcast_to(ids[...], (tokens, tokens))
        return jnp.sum(jnp.where(row == column, spread, 0), axis=1, keepdims=True)

    def block(slot, head, source, allowed, first):
        rows = slot_rows(slot)
        columns = slice(head * HEAD, (head + 1) * HEAD)
        lanes = slice(head * 128, (head + 1) * 128)
        scores = lax.dot_general(
            qry[rows, columns], source[rows, :HEAD], (((1,), (1,)), ((), ())),
            preferred_element_type=jnp.float32,
        )
        bent = jnp.tanh(scores * (1.0 / (math.sqrt(HEAD) * CAP)))
        weights = jnp.where(allowed, jnp.exp2(bent * (CAP * math.log2(math.e))), 0.0)
        total = jnp.broadcast_to(jnp.sum(weights, axis=1, keepdims=True), (tokens, 128))
        mixed = jnp.dot(
            weights.astype(jnp.bfloat16), source[rows, HEAD:], preferred_element_type=jnp.float32
        )
        if first:
            acc[rows, columns] = mixed
            tot[rows, lanes] = total
        else:
            acc[rows, columns] += mixed
            tot[rows, lanes] += total

    def blocks(slot, source, allowed, first):
        for head in range(group):
            block(slot, head, source, allowed, first)

    def own_block(slot):
        ids = (ids0, ids1)[slot]
        blocks(slot, kv, (column <= row) & (as_column(ids) == ids[...]), True)

    def far_block(slot):
        ids = as_column((ids0, ids1)[slot])
        blocks(slot, kv2, (ids == (far0, far1)[slot][...]) & (row + seq >= row + 2), False)

    def near_block(slot):
        ids = as_column((ids0, ids1)[slot])
        blocks(slot, kv1, (ids == (near0, near1)[slot][...]) & (row + seq >= row + 1), False)
        rows = slot_rows(slot)
        for head in range(group):
            columns = slice(head * HEAD, (head + 1) * HEAD)
            att[rows, columns] = (acc[rows, columns] / tot[rows, head * 128 : head * 128 + 1]).astype(
                jnp.bfloat16
            )

    own_copies[0].wait()
    for moving in table_copies:
        moving.wait()
    normalize(own, 0, 0, tokens)
    gather_q.step(1, early, early_relay)
    ids_across.wait()
    ids_after[1].start()
    positions = seq * tokens + lax.broadcasted_iota(jnp.int32, cos.shape, 0)
    angles = positions.astype(jnp.float32) * inverse[...]
    cos[...] = jnp.cos(angles)
    sin[...] = jnp.sin(angles)

    @pl.when(chip == 0)
    def _():
        kv2[...] = jnp.zeros_like(kv2)

    gather_q.step(2, early, early_relay)
    gather_q.first(late)
    for hop in range(3, gather_q.near + 1):
        gather_q.step(hop, early, early_relay)
    for moving in own_copies[1:]:
        moving.wait()
    for hop in range(gather_q.near + 1, gather_q.far + 1):
        gather_q.step(hop, early, early_relay)
    gather_o.first(crossers)
    gather_q.step(1, late, late_relay)
    gather_q.arrived(wq.at[:2, : chips * rows_q, :], early_relay)
    gather_o.first(others)
    make_kv(0)
    gather_q.step(2, late, late_relay)
    take_guest(0)
    gather_o.step(1, crossers, o_relay, over)
    take_guest(1)
    for hop in range(3, gather_q.near + 1):
        gather_q.step(hop, late, late_relay)
    gather_o.step(1, others, o_relay)
    take_guest(2)
    take_guest(3)
    make_kv(1)
    send_kv(1)
    gather_o.step(2, crossers, o_relay, over)
    send_kv(0)
    gather_o.step(2, others, o_relay)
    ids_near()
    for hop in range(gather_q.near + 1, gather_q.far + 1):
        gather_q.step(hop, late, late_relay)
    gather_q.arrived(wq.at[2:, : chips * rows_q, :], late_relay)
    make_queries(1)
    own_block(1)
    make_queries(0)
    own_block(0)
    small(ids0, near0, 3, sibling).wait()
    small(ids1, near1, 4, sibling).wait()
    take_kv(1)
    far_block(1)
    for hop in range(3, gather_o.near + 1):
        gather_o.step(hop, crossers, o_relay, over)
    take_near(1)
    near_block(1)
    att_moving = small(att.at[slot_rows(1), :], attx, 9, across)
    att_moving.start()
    for hop in range(3, gather_o.near + 1):
        gather_o.step(hop, others, o_relay)
    take_kv(0)
    far_block(0)
    for hop in range(gather_o.near + 1, gather_o.far + 1):
        gather_o.step(hop, crossers, o_relay, over)
    take_near(0)
    near_block(0)
    for hop in range(1, gather_o.far):
        crossed(hop, crossers)
    for hop in range(gather_o.near + 1, gather_o.far + 1):
        gather_o.step(hop, others, o_relay)
    crossed(gather_o.far, crossers)
    gather_o.arrived(wo.at[: chips * rows_o, :], o_relay)
    mine_at = pl.ds(pl.multiple_of(x * group * HEAD, HEAD), group * HEAD)
    theirs_at = pl.ds(pl.multiple_of((1 - x) * group * HEAD, HEAD), group * HEAD)
    chunks = [slice(start, start + 256) for start in range(0, width, 256)]
    for chunk in chunks:
        branch[:, chunk] = jnp.dot(
            att[slot_rows(0), :], wo[mine_at, chunk], preferred_element_type=jnp.float32
        )
    att_moving.wait()
    for chunk in chunks:
        branch[:, chunk] += jnp.dot(
            attx[...], wo[theirs_at, chunk], preferred_element_type=jnp.float32
        )

    for slot in range(2):
        @pl.when(chip < chips - 1)
        def _():
            kv_moving(slot).wait_send()
    gather_q.sent(wq.at[:, : (2 * chips - 1) * rows_q, :])
    gather_o.sent(wo.at[: (2 * chips - 1) * rows_o, :])


def finish_kernel(own, branch, post, result, out, sems):
    tokens = own.shape[0]
    strip, portion = 16, tokens // 4
    leaving = []
    for index in range(4):
        @pl.loop(index * portion // strip, (index + 1) * portion // strip, unroll=2)
        def _(step):
            rows = pl.ds(pl.multiple_of(step * strip, strip), strip)
            scaled = rms_scale(branch[rows, :], post[...])
            out[rows, :] = (own[rows, :].astype(jnp.float32) + scaled).astype(jnp.bfloat16)

        part = pl.ds(index * portion, portion)
        leaving.append(pltpu.make_async_copy(out.at[part, :], result.at[part, :], sems.at[index]))
        leaving[-1].start()
    for moving in leaving:
        moving.wait()


def paired_layer(hidden_in, segment_ids, pre_gain, w_qkv, w_out, post_gain):
    tokens, width = hidden_in.shape[1:]
    chips = lax.axis_size("seq") // 2
    bf16, f32 = jnp.bfloat16, jnp.float32
    steps = np.arange(HEAD // 2, dtype=np.float32) * np.float32(2.0 / HEAD)
    inverse = np.float32(1.0) / np.float32(10000.0) ** steps
    vmem, dma = pltpu.VMEM, pltpu.SemaphoreType.DMA
    group = Q_HEADS // KV_HEADS
    heads = group * HEAD
    q_sems = 2 * (2 + group) * (chips - 1) + 2
    o_sems = 6 * (chips - 1) + 1
    anywhere = pl.BlockSpec(memory_space=pl.ANY)
    in_vmem = pl.BlockSpec(memory_space=vmem)
    own, branch = pl.pallas_call(
        functools.partial(layer_kernel, chips),
        out_shape=(vmem((tokens, width), bf16), vmem((tokens, width), f32)),
        in_specs=[anywhere] * 6,
        out_specs=(in_vmem, in_vmem),
        scratch_shapes=[
            vmem((1, tokens), jnp.int32),
            vmem((1, HEAD // 2), f32),
            vmem((width,), f32),
            vmem((2 + group, width, HEAD), bf16),
            vmem((w_out.shape[0] * chips * 2, width), bf16),
            vmem((tokens, width), bf16),
            vmem((2 * tokens, width), bf16),
            vmem((2 * tokens, heads), bf16),
            vmem((2 * tokens, 2 * HEAD), bf16),
            vmem((2 * tokens, 2 * HEAD), bf16),
            vmem((2 * tokens, 2 * HEAD), bf16),
            vmem((1, tokens), jnp.int32),
            vmem((1, tokens), jnp.int32),
            vmem((1, tokens), jnp.int32),
            vmem((1, tokens), jnp.int32),
            vmem((1, tokens), jnp.int32),
            vmem((tokens, HEAD // 2), f32),
            vmem((tokens, HEAD // 2), f32),
            vmem((2 * tokens, heads), f32),
            vmem((2 * tokens, group * 128), f32),
            vmem((2 * tokens, heads), bf16),
            vmem((tokens, heads), bf16),
            dma((1,)),
            dma((q_sems,)),
            dma((1,)),
            dma((o_sems,)),
            dma((14,)),
            dma((14,)),
            dma((7 + group,)),
        ],
        compiler_params=pltpu.CompilerParams(
            collective_id=0, has_side_effects=True, vmem_limit_bytes=58 * 1024 * 1024
        ),
    )(
        hidden_in[0],
        segment_ids,
        jnp.asarray(inverse)[None, :],
        pre_gain,
        w_qkv,
        w_out,
    )
    result = pl.pallas_call(
        finish_kernel,
        out_shape=jax.ShapeDtypeStruct((tokens, width), bf16),
        in_specs=[in_vmem] * 3,
        out_specs=anywhere,
        scratch_shapes=[vmem((tokens, width), bf16), dma((4,))],
        compiler_params=pltpu.CompilerParams(vmem_limit_bytes=12 * 1024 * 1024),
    )(
        pltpu.with_memory_space_constraint(own, vmem),
        pltpu.with_memory_space_constraint(branch, vmem),
        post_gain,
    )
    return result[None]


def per_device(hidden_in, segment_ids, pre_gain, w_qkv, w_out, post_gain):
    tokens, width = hidden_in.shape[1:]
    seq_count = lax.axis_size("seq")
    doc_most = min(WINDOW, seq_count * tokens // 8)
    whole_tiles = w_qkv.shape[0] % 16 == 0 and w_out.shape[0] % 16 == 0 and width % 768 == 0
    two_hops = doc_most - 1 <= 2 * tokens and 3 * tokens <= WINDOW
    small_ring = seq_count % 4 == 0 and seq_count > 12
    if whole_tiles and two_hops and small_ring and lax.axis_size("batch") == 2 and KV_HEADS == 2:
        layer = paired_layer
    else:
        layer = plain_layer
    return layer(hidden_in, segment_ids, pre_gain, w_qkv, w_out, post_gain)


def solution(mesh):
    placed = (P("batch", "seq", None), P("batch", "seq"), P(), P("seq", None), P("seq", None), P())
    return jax.shard_map(
        per_device, mesh=mesh, in_specs=placed, out_specs=P("batch", "seq", None), check_vma=False
    )
```

```python
import functools
import math

import jax
import jax.numpy as jnp
import numpy as np
from jax import lax
from jax.experimental import pallas as pl
from jax.experimental.pallas import tpu as pltpu
from jax.sharding import PartitionSpec as P

Q_HEADS = 4
KV_HEADS = 2
HEAD = 256
WINDOW = 4096
DOCS = 16


EPS = 1e-06
CAP = 50.0


def from_behind(block, axis, distance):
    devices = range(lax.axis_size(axis))
    route = [(i - distance, i) for i in devices if i - distance in devices]
    return lax.ppermute(block, axis, route)


def rms_scale(values, gain):
    return values * lax.rsqrt(jnp.mean(values * values, axis=-1, keepdims=True) + EPS) * gain


def rotary(values, positions, leading):
    head_size = values.shape[-1]
    half_dim = head_size // 2
    inverse = 1.0 / 10000.0 ** (jnp.arange(half_dim, dtype=jnp.float32) * 2.0 / head_size)
    angles = positions.astype(jnp.float32)[:, None] * inverse[None, :]
    shape = (
        (1,) * leading + (positions.shape[0],) + (1,) * (values.ndim - 2 - leading) + (half_dim,)
    )
    cosine = jnp.cos(angles).reshape(shape)
    sine = jnp.sin(angles).reshape(shape)
    first_half = values[..., :half_dim]
    second_half = values[..., half_dim:]
    return jnp.concatenate(
        [first_half * cosine - second_half * sine, second_half * cosine + first_half * sine],
        axis=-1,
    )


def plain_layer(hidden_in, segment_ids, pre_gain, w_qkv, w_out, post_gain):
    tok_rows = hidden_in.shape[1]
    seq_count = lax.axis_size("seq")
    seq_index = lax.axis_index("seq")
    groups = Q_HEADS // KV_HEADS
    doc_most = min(WINDOW, seq_count * tok_rows // 8)
    hops = min(-(-(doc_most - 1) // tok_rows), seq_count - 1)
    positions = seq_index * tok_rows + jnp.arange(tok_rows, dtype=jnp.int32)
    own_ids = segment_ids[0]
    id_blocks = [from_behind(own_ids, "seq", d) for d in range(hops, 0, -1)] + [own_ids]
    widened = hidden_in[0].astype(jnp.float32)
    normed = rms_scale(widened, pre_gain).astype(jnp.bfloat16)
    projected = jnp.dot(
        normed,
        lax.all_gather(w_qkv, "seq", axis=0, tiled=True),
        preferred_element_type=jnp.float32,
    )
    queries = rotary(
        projected[:, : Q_HEADS * HEAD].reshape(tok_rows, KV_HEADS, groups, HEAD), positions, 0
    ).astype(jnp.bfloat16)
    key_rows = rotary(
        projected[:, Q_HEADS * HEAD : (Q_HEADS + KV_HEADS) * HEAD].reshape(
            tok_rows, KV_HEADS, HEAD
        ),
        positions,
        0,
    ).astype(jnp.bfloat16)
    value_rows = projected[:, (Q_HEADS + KV_HEADS) * HEAD :].astype(jnp.bfloat16)
    both = jnp.concatenate([key_rows.reshape(tok_rows, KV_HEADS * HEAD), value_rows], axis=1)
    blocks = [from_behind(both, "seq", d) for d in range(hops, 0, -1)] + [both]
    kv = jnp.concatenate(blocks, axis=0).reshape(-1, 2, KV_HEADS, HEAD)
    ids = jnp.concatenate(id_blocks, axis=0)
    key_pos = (seq_index - hops) * tok_rows + jnp.arange((hops + 1) * tok_rows, dtype=jnp.int32)
    allowed = (
        (key_pos[None, :] >= 0)
        & (key_pos[None, :] <= positions[:, None])
        & (positions[:, None] - key_pos[None, :] < WINDOW)
        & (ids[None, :] == own_ids[:, None])
    )
    scores = jnp.einsum(
        "qhgd,khd->hgqk", queries, kv[:, 0], preferred_element_type=jnp.float32
    ) * (1.0 / math.sqrt(HEAD))
    capped = CAP * jnp.tanh(scores / CAP)
    weights = jnp.where(allowed[None, None], jnp.exp(capped), 0.0)
    totals = jnp.sum(weights, axis=-1)
    mixed = jnp.einsum(
        "hgqk,khd->hgqd", weights.astype(jnp.bfloat16), kv[:, 1], preferred_element_type=jnp.float32
    )
    attended = (mixed / totals[..., None]).astype(jnp.bfloat16)
    attended = attended.transpose(2, 0, 1, 3).reshape(tok_rows, Q_HEADS * HEAD)
    branch = jnp.dot(
        attended,
        lax.all_gather(w_out, "seq", axis=0, tiled=True),
        preferred_element_type=jnp.float32,
    )
    return (widened + rms_scale(branch, post_gain)).astype(jnp.bfloat16)[None]


def split_rows(rows):
    first = (rows // 16 + 1) // 2 * 16
    return ((0, first), (first, rows - first))


class Ring:
    def __init__(self, place, classes, own_spot, full_spot, send_sem, recv_sems):
        self.place, self.classes = place, classes
        self.own_spot, self.full_spot = own_spot, full_spot
        self.send_sem, self.recv_sems = send_sem, recv_sems
        self.far = place["chips"] // 2
        self.near = place["chips"] - 1 - self.far
        self.extra = len(classes) * (self.far + self.near)

    def reach(self, piece, way):
        return self.far if self.classes[piece] == way else self.near

    def slot(self, piece, way, hop):
        onset = 0 if self.classes[piece] == way else self.far
        return piece * (self.far + self.near) + onset + hop - 1

    def origin(self, way, hop):
        return self.place["chip_at"](self.place["ring"] + (hop if way else -hop))

    def spot(self, piece, way, hop):
        return self.full_spot(piece, self.origin(way, hop) * 2 + self.place["core"])

    def copy(self, source, target, slot, device):
        return pltpu.make_async_remote_copy(
            src_ref=source,
            dst_ref=target,
            send_sem=self.send_sem.at[0],
            recv_sem=self.recv_sems.at[slot],
            device_id=device,
            device_id_type=pl.DeviceIdType.MESH,
        )

    def send(self, source, target, slot, device):
        self.copy(source, target, slot, device).start()

    def arrived(self, spot, slot):
        self.copy(spot, spot, slot, self.place["sibling"]).wait_recv()

    def sent(self, as_much):
        self.copy(as_much, as_much, 0, self.place["sibling"]).wait_send()

    def first(self, pieces):
        for piece in pieces:
            for way in (0, 1):
                self.send(
                    self.own_spot(piece),
                    self.full_spot(piece, self.place["seq"]),
                    self.slot(piece, way, 1),
                    self.place["onward"][way],
                )

    def step(self, hop, pieces, relay_slot, then=None):
        place = self.place
        for piece in pieces:
            for way in (0, 1):
                if hop > self.reach(piece, way):
                    continue
                spot = self.spot(piece, way, hop)
                slot = self.slot(piece, way, hop)
                self.arrived(spot, slot)
                if hop < self.reach(piece, way):
                    self.send(spot, spot, slot + 1, place["onward"][way])
                if then is not None:
                    then(piece, way, hop, spot)
                self.send(spot, spot, relay_slot, place["sibling"])


def layer_kernel(
    chips, hid, ids, inverse_in, pre_in, w_qkv, w_out, own, branch,
    ids0, inverse, pre, wq, wo, guest, nrm, qry, kv, kv1, kv2, ids1, far0, far1, near0, near1,
    cos, sin, acc, tot, att, attx,
    q_send, q_recv, o_send, o_recv, s_send, s_recv, local_sem,
):
    seq, x = lax.axis_index("seq"), lax.axis_index("batch")
    chip, core = seq // 2, seq % 2
    half = chips // 2
    layer, side = chip // 2, chip % 2
    ring = (1 - side) * layer + side * (chips - 1 - layer)

    def chip_at(position):
        position = (position + chips) % chips
        far = position // half
        return (1 - far) * 2 * position + far * (2 * (chips - 1 - position) + 1)

    def at(device_chip, device_core, batch):
        return {"seq": device_chip * 2 + device_core, "batch": batch}

    up, down = at(chip_at(ring + 1), core, x), at(chip_at(ring - 1), core, x)
    sibling, across = at(chip, 1 - core, x), at(chip, core, 1 - x)
    after = at((chip + 1) % chips, core, x)
    before = at((chip + chips - 1) % chips, core, x)
    place = dict(
        chips=chips, seq=seq, core=core, ring=ring, chip_at=chip_at, sibling=sibling,
        onward=(up, down),
    )
    tokens, width = own.shape
    rows_q, rows_o = w_qkv.shape[0], w_out.shape[0]
    group = Q_HEADS // KV_HEADS
    third_width = width // 6

    def local(source, target, slot):
        moving = pltpu.make_async_copy(source, target, local_sem.at[slot])
        moving.start()
        return moving

    column_at = [
        (Q_HEADS + x) * HEAD, (Q_HEADS + KV_HEADS + x) * HEAD
    ] + [(group * x + head) * HEAD for head in range(group)]

    def columns_of(kind):
        return pl.ds(pl.multiple_of(column_at[kind], HEAD), HEAD)

    kinds = len(column_at)
    q_pieces = [(kind, start, count) for kind in range(kinds) for start, count in split_rows(rows_q)]

    def q_own(piece):
        kind, start, count = q_pieces[piece]
        return w_qkv.at[pl.ds(start, count), columns_of(kind)]

    def q_full(piece, device):
        kind, start, count = q_pieces[piece]
        return wq.at[kind, pl.ds(pl.multiple_of(device * rows_q + start, 16), count), :]

    def q_rows(kind, device):
        return wq.at[kind, pl.ds(pl.multiple_of(device * rows_q, 16), rows_q), :]

    def o_columns(third, unit):
        return pl.ds(pl.multiple_of((third * 2 + unit) * third_width, 128), third_width)

    def o_rows(device):
        return pl.ds(pl.multiple_of(device * rows_o, 16), rows_o)

    o_thirds = (2 * x, 1)

    def o_own(piece):
        return w_out.at[:, o_columns(o_thirds[piece % 2], piece // 2)]

    def o_full(piece, device):
        return wo.at[o_rows(device), o_columns(o_thirds[piece % 2], piece // 2)]

    gather_q = Ring(place, [kind % 2 for kind, _, _ in q_pieces], q_own, q_full, q_send, q_recv)
    gather_o = Ring(place, [0, 1, 0, 1], o_own, o_full, o_send, o_recv)

    ids_copy = local(ids, ids0, kinds + 2)
    own_copies = [local(hid, own, 0)]
    table_copies = [
        local(source, target, kinds + 3 + index)
        for index, (source, target) in enumerate(((inverse_in, inverse), (pre_in, pre)))
    ]
    for kind in range(kinds):
        own_copies.append(local(w_qkv.at[:, columns_of(kind)], q_rows(kind, seq), kind + 1))
    own_copies.append(local(w_out, wo.at[o_rows(seq), :], kinds + 1))

    met = [sibling, across, up, down, after, before]
    barrier = pltpu.get_barrier_semaphore()
    for other in met:
        pl.semaphore_signal(barrier, 1, device_id=other, device_id_type=pl.DeviceIdType.MESH)
    ids_copy.wait()
    pl.semaphore_wait(barrier, len(met))

    def small(source, target, slot, device):
        return pltpu.make_async_remote_copy(
            src_ref=source, dst_ref=target, send_sem=s_send.at[slot], recv_sem=s_recv.at[slot],
            device_id=device, device_id_type=pl.DeviceIdType.MESH,
        )

    early = [piece for piece in range(len(q_pieces)) if q_pieces[piece][0] < 2]
    late = [piece for piece in range(len(q_pieces)) if q_pieces[piece][0] >= 2]
    crossers, others = (0, 2), (1, 3)
    early_relay, late_relay, o_relay = gather_q.extra, gather_q.extra + 1, gather_o.extra
    o_pieces = crossers + others
    ids_across = small(ids0, ids1, 0, across)
    ids_across.start()
    ids_after = [small(ids0, far0, 1, after), small(ids1, far1, 2, after)]
    ids_after[0].start()
    gather_q.first(early)
    portion = tokens // 4
    guests = []
    for index in range(4):
        part = pl.ds(index * portion, portion)
        guests.append(small(hid.at[part, :], guest.at[part, :], 10 + index, across))
        guests[-1].start()
    for kind in range(kinds):
        gather_q.send(
            w_qkv.at[:, columns_of(kind)], q_rows(kind, seq), early_relay + (kind >= 2), sibling
        )
    gather_o.send(w_out, wo.at[o_rows(seq), :], o_relay, sibling)

    strip = 16

    def normalize(source, base, start, count):
        @pl.loop(0, count // strip, unroll=2)
        def _(index):
            at_row = pl.multiple_of(start + index * strip, strip)
            values = source[pl.ds(at_row, strip), :].astype(jnp.float32)
            nrm[pl.ds(pl.multiple_of(base + at_row, strip), strip), :] = rms_scale(
                values, pre[...]
            ).astype(jnp.bfloat16)

    def pass_on(mine, far, near, slot):
        @pl.when(core == 0)
        def _():
            small(mine, near, slot, sibling).start()

        @pl.when(core == 1)
        def _():
            small(far, near, slot, sibling).start()

    def ids_near():
        ids_after[0].wait()
        ids_after[1].wait()
        pass_on(ids0, far0, near0, 3)
        pass_on(ids1, far1, near1, 4)

    def slot_rows(slot):
        return pl.ds(slot * tokens, tokens)

    def project(slot, kind):
        return jnp.dot(nrm[slot_rows(slot), :], wq[kind], preferred_element_type=jnp.float32)

    def turned(values):
        a, b = values[:, : HEAD // 2], values[:, HEAD // 2 :]
        c, s = cos[...], sin[...]
        return jnp.concatenate([a * c - b * s, b * c + a * s], axis=1).astype(jnp.bfloat16)

    def kv_moving(slot):
        return small(kv.at[slot_rows(slot), :], kv2.at[slot_rows(slot), :], 5 + slot, after)

    def make_kv(slot):
        kv[slot_rows(slot), :HEAD] = turned(project(slot, 0))
        kv[slot_rows(slot), HEAD:] = project(slot, 1).astype(jnp.bfloat16)

    def send_kv(slot):
        @pl.when(chip < chips - 1)
        def _():
            kv_moving(slot).start()

    def take_kv(slot):
        @pl.when(chip > 0)
        def _():
            kv_moving(slot).wait_recv()

        rows = slot_rows(slot)
        pass_on(kv.at[rows, :], kv2.at[rows, :], kv1.at[rows, :], 7 + slot)

    def take_near(slot):
        rows = slot_rows(slot)
        small(kv.at[rows, :], kv1.at[rows, :], 7 + slot, sibling).wait()

    def make_queries(slot):
        for head in range(group):
            qry[slot_rows(slot), head * HEAD : (head + 1) * HEAD] = turned(project(slot, 2 + head))

    def take_guest(index):
        guests[index].wait()
        normalize(guest, tokens, index * portion, portion)

    def over(piece, way, hop, spot):
        if piece in crossers:
            gather_o.send(spot, spot, crossing(piece, way, hop), across)

    def crossing(piece, way, hop):
        first = crossers.index(piece) - piece
        return o_relay + 1 + first * (chips - 1) + gather_o.slot(piece, way, hop)

    def crossed(hop, pieces):
        for piece in pieces:
            for way in (0, 1):
                if hop > gather_o.reach(piece, way):
                    continue
                device = gather_o.origin(way, hop) * 2 + core
                spot = wo.at[o_rows(device), o_columns(2 - 2 * x, piece // 2)]
                gather_o.arrived(spot, crossing(piece, way, hop))
                gather_o.send(spot, spot, o_relay, sibling)

    row = lax.broadcasted_iota(jnp.int32, (tokens, tokens), 0)
    column = lax.broadcasted_iota(jnp.int32, (tokens, tokens), 1)

    def as_column(ids):
        spread = jnp.broadcast_to(ids[...], (tokens, tokens))
        return jnp.sum(jnp.where(row == column, spread, 0), axis=1, keepdims=True)

    def block(slot, head, source, allowed, first):
        rows = slot_rows(slot)
        columns = slice(head * HEAD, (head + 1) * HEAD)
        lanes = slice(head * 128, (head + 1) * 128)
        scores = lax.dot_general(
            qry[rows, columns], source[rows, :HEAD], (((1,), (1,)), ((), ())),
            preferred_element_type=jnp.float32,
        )
        bent = jnp.tanh(scores * (1.0 / (math.sqrt(HEAD) * CAP)))
        weights = jnp.where(allowed, jnp.exp2(bent * (CAP * math.log2(math.e))), 0.0)
        total = jnp.broadcast_to(jnp.sum(weights, axis=1, keepdims=True), (tokens, 128))
        mixed = jnp.dot(
            weights.astype(jnp.bfloat16), source[rows, HEAD:], preferred_element_type=jnp.float32
        )
        if first:
            acc[rows, columns] = mixed
            tot[rows, lanes] = total
        else:
            acc[rows, columns] += mixed
            tot[rows, lanes] += total

    def blocks(slot, source, allowed, first):
        for head in range(group):
            block(slot, head, source, allowed, first)

    def own_block(slot):
        ids = (ids0, ids1)[slot]
        blocks(slot, kv, (column <= row) & (as_column(ids) == ids[...]), True)

    def far_block(slot):
        ids = as_column((ids0, ids1)[slot])
        blocks(slot, kv2, (ids == (far0, far1)[slot][...]) & (row + seq >= row + 2), False)

    def near_block(slot):
        ids = as_column((ids0, ids1)[slot])
        blocks(slot, kv1, (ids == (near0, near1)[slot][...]) & (row + seq >= row + 1), False)
        rows = slot_rows(slot)
        for head in range(group):
            columns = slice(head * HEAD, (head + 1) * HEAD)
            att[rows, columns] = (acc[rows, columns] / tot[rows, head * 128 : head * 128 + 1]).astype(
                jnp.bfloat16
            )

    own_copies[0].wait()
    for moving in table_copies:
        moving.wait()
    normalize(own, 0, 0, tokens)
    gather_q.step(1, early, early_relay)
    ids_across.wait()
    ids_after[1].start()
    positions = seq * tokens + lax.broadcasted_iota(jnp.int32, cos.shape, 0)
    angles = positions.astype(jnp.float32) * inverse[...]
    cos[...] = jnp.cos(angles)
    sin[...] = jnp.sin(angles)

    @pl.when(chip == 0)
    def _():
        kv2[...] = jnp.zeros_like(kv2)

    gather_q.step(2, early, early_relay)
    gather_q.first(late)
    for hop in range(3, gather_q.near + 1):
        gather_q.step(hop, early, early_relay)
    for moving in own_copies[1:]:
        moving.wait()
    for hop in range(gather_q.near + 1, gather_q.far + 1):
        gather_q.step(hop, early, early_relay)
    gather_o.first(crossers)
    gather_q.step(1, late, late_relay)
    gather_q.arrived(wq.at[:2, : chips * rows_q, :], early_relay)
    gather_o.first(others)
    make_kv(0)
    gather_q.step(2, late, late_relay)
    take_guest(0)
    gather_o.step(1, crossers, o_relay, over)
    take_guest(1)
    gather_q.step(3, late, late_relay)
    take_guest(2)
    take_guest(3)
    make_kv(1)
    send_kv(1)
    gather_o.step(1, others, o_relay)
    gather_o.step(2, crossers, o_relay, over)
    send_kv(0)
    ids_near()
    gather_q.step(4, late, late_relay)
    gather_q.arrived(wq.at[2:, : chips * rows_q, :], late_relay)
    make_queries(1)
    own_block(1)
    make_queries(0)
    own_block(0)
    gather_o.step(2, others, o_relay)
    small(ids0, near0, 3, sibling).wait()
    small(ids1, near1, 4, sibling).wait()
    take_kv(1)
    far_block(1)
    gather_o.step(3, crossers, o_relay, over)
    take_near(1)
    near_block(1)
    att_moving = small(att.at[slot_rows(1), :], attx, 9, across)
    att_moving.start()
    gather_o.step(3, others, o_relay)
    take_kv(0)
    far_block(0)
    gather_o.step(4, crossers, o_relay, over)
    take_near(0)
    near_block(0)
    crossed(1, crossers)
    crossed(2, crossers)
    crossed(3, crossers)
    gather_o.step(4, others, o_relay)
    crossed(4, crossers)
    gather_o.arrived(wo.at[: chips * rows_o, :], o_relay)
    mine_at = pl.ds(pl.multiple_of(x * group * HEAD, HEAD), group * HEAD)
    theirs_at = pl.ds(pl.multiple_of((1 - x) * group * HEAD, HEAD), group * HEAD)
    chunks = [slice(start, start + 256) for start in range(0, width, 256)]
    for chunk in chunks:
        branch[:, chunk] = jnp.dot(
            att[slot_rows(0), :], wo[mine_at, chunk], preferred_element_type=jnp.float32
        )
    att_moving.wait()
    for chunk in chunks:
        branch[:, chunk] += jnp.dot(
            attx[...], wo[theirs_at, chunk], preferred_element_type=jnp.float32
        )

    for slot in range(2):
        @pl.when(chip < chips - 1)
        def _():
            kv_moving(slot).wait_send()
    gather_q.sent(wq.at[:, : (2 * chips - 1) * rows_q, :])
    gather_o.sent(wo.at[: (2 * chips - 1) * rows_o, :])


def finish_kernel(own, branch, post, result, out, sems):
    tokens = own.shape[0]
    strip, portion = 16, tokens // 4
    leaving = []
    for index in range(4):
        @pl.loop(index * portion // strip, (index + 1) * portion // strip, unroll=2)
        def _(step):
            rows = pl.ds(pl.multiple_of(step * strip, strip), strip)
            scaled = rms_scale(branch[rows, :], post[...])
            out[rows, :] = (own[rows, :].astype(jnp.float32) + scaled).astype(jnp.bfloat16)

        part = pl.ds(index * portion, portion)
        leaving.append(pltpu.make_async_copy(out.at[part, :], result.at[part, :], sems.at[index]))
        leaving[-1].start()
    for moving in leaving:
        moving.wait()


def paired_layer(hidden_in, segment_ids, pre_gain, w_qkv, w_out, post_gain):
    tokens, width = hidden_in.shape[1:]
    chips = lax.axis_size("seq") // 2
    bf16, f32 = jnp.bfloat16, jnp.float32
    steps = np.arange(HEAD // 2, dtype=np.float32) * np.float32(2.0 / HEAD)
    inverse = np.float32(1.0) / np.float32(10000.0) ** steps
    vmem, dma = pltpu.VMEM, pltpu.SemaphoreType.DMA
    group = Q_HEADS // KV_HEADS
    heads = group * HEAD
    q_sems = 2 * (2 + group) * (chips - 1) + 2
    o_sems = 6 * (chips - 1) + 1
    anywhere = pl.BlockSpec(memory_space=pl.ANY)
    in_vmem = pl.BlockSpec(memory_space=vmem)
    own, branch = pl.pallas_call(
        functools.partial(layer_kernel, chips),
        out_shape=(vmem((tokens, width), bf16), vmem((tokens, width), f32)),
        in_specs=[anywhere] * 6,
        out_specs=(in_vmem, in_vmem),
        scratch_shapes=[
            vmem((1, tokens), jnp.int32),
            vmem((1, HEAD // 2), f32),
            vmem((width,), f32),
            vmem((2 + group, width, HEAD), bf16),
            vmem((w_out.shape[0] * chips * 2, width), bf16),
            vmem((tokens, width), bf16),
            vmem((2 * tokens, width), bf16),
            vmem((2 * tokens, heads), bf16),
            vmem((2 * tokens, 2 * HEAD), bf16),
            vmem((2 * tokens, 2 * HEAD), bf16),
            vmem((2 * tokens, 2 * HEAD), bf16),
            vmem((1, tokens), jnp.int32),
            vmem((1, tokens), jnp.int32),
            vmem((1, tokens), jnp.int32),
            vmem((1, tokens), jnp.int32),
            vmem((1, tokens), jnp.int32),
            vmem((tokens, HEAD // 2), f32),
            vmem((tokens, HEAD // 2), f32),
            vmem((2 * tokens, heads), f32),
            vmem((2 * tokens, group * 128), f32),
            vmem((2 * tokens, heads), bf16),
            vmem((tokens, heads), bf16),
            dma((1,)),
            dma((q_sems,)),
            dma((1,)),
            dma((o_sems,)),
            dma((14,)),
            dma((14,)),
            dma((7 + group,)),
        ],
        compiler_params=pltpu.CompilerParams(
            collective_id=0, has_side_effects=True, vmem_limit_bytes=58 * 1024 * 1024
        ),
    )(
        hidden_in[0],
        segment_ids,
        jnp.asarray(inverse)[None, :],
        pre_gain,
        w_qkv,
        w_out,
    )
    result = pl.pallas_call(
        finish_kernel,
        out_shape=jax.ShapeDtypeStruct((tokens, width), bf16),
        in_specs=[in_vmem] * 3,
        out_specs=anywhere,
        scratch_shapes=[vmem((tokens, width), bf16), dma((4,))],
        compiler_params=pltpu.CompilerParams(vmem_limit_bytes=12 * 1024 * 1024),
    )(
        pltpu.with_memory_space_constraint(own, vmem),
        pltpu.with_memory_space_constraint(branch, vmem),
        post_gain,
    )
    return result[None]


def per_device(hidden_in, segment_ids, pre_gain, w_qkv, w_out, post_gain):
    tokens, width = hidden_in.shape[1:]
    seq_count = lax.axis_size("seq")
    doc_most = min(WINDOW, seq_count * tokens // 8)
    whole_tiles = w_qkv.shape[0] % 16 == 0 and w_out.shape[0] % 16 == 0 and width % 768 == 0
    two_hops = doc_most - 1 <= 2 * tokens and 3 * tokens <= WINDOW
    small_ring = seq_count % 4 == 0 and seq_count > 12
    if whole_tiles and two_hops and small_ring and lax.axis_size("batch") == 2 and KV_HEADS == 2:
        layer = paired_layer
    else:
        layer = plain_layer
    return layer(hidden_in, segment_ids, pre_gain, w_qkv, w_out, post_gain)


def solution(mesh):
    placed = (P("batch", "seq", None), P("batch", "seq"), P(), P("seq", None), P("seq", None), P())
    return jax.shard_map(
        per_device, mesh=mesh, in_specs=placed, out_specs=P("batch", "seq", None), check_vma=False
    )
```
